32 devices in a mesh: owner: 4 (over x, core), rows: 8 (over z, y).
Axes of the slice: x: 2, y: 2, z: 4, core: 2. Of those that a mesh axis runs over, the one named last changes fastest.
Arguments:
- train_gate: float32 [128, 2048, 768], P('owner', 'rows'), may hold values from -0.1875 to 0.1875
- train_up: float32 [128, 2048, 768], P('owner', 'rows'), may hold values from -0.1875 to 0.1875
- router_weight: float32 [2048, 128], P('rows', 'owner'), may hold values from -0.125 to 0.125
- router_gain: float32 [2048], P('rows'), may hold values from 0.25 to 1.75
Outputs:
- ready_gate: bfloat16 [128, 2048, 768], P(('owner', 'rows'))
- ready_up: bfloat16 [128, 2048, 768], P(('owner', 'rows'))
- scale_gate: float32 [128, 768], P(('owner', 'rows'))
- scale_up: float32 [128, 768], P(('owner', 'rows'))
- serve_router: bfloat16 [2048, 128], replicated
The draws below stay inside these ranges and needn't reach their ends.
All inputs are finite; a program needn't handle non-finite values.
Results may differ from the reference program's by a relative error of at most 0.001.
Values may be sent and summed in bfloat16 or wider, within the bound.
No kernel may reach another device: no remote copies, remote signals or barrier semaphores. Data moves between devices by JAX's collectives and lax.ppermute only.
A program may use at most 192 MiB of HBM per device.

```python
import jax
import jax.numpy as jnp
from jax import lax

EXPERTS = 128
D_MODEL = 2048
D_EXPERT = 768


def spiked(drawn, rng, source, target, parts, factor):
    def block_of(position):
        return (jnp.arange(drawn.shape[position]) // (drawn.shape[position] // parts)).reshape((-1,) + (1,) * (drawn.ndim - 1 - position))

    near = jax.random.permutation(rng, parts)[block_of(target)]
    other_side = (block_of(target) + parts // 2) % parts
    return jnp.where((block_of(source) == near) | (block_of(source) == other_side), factor * drawn, drawn)


def shard_levels(key, dims, cuts, low, high):
    loudness, own = 1.0, jax.random.fold_in(key, 6)
    for axis_at, blocks in cuts:
        heights = jnp.exp(jax.random.uniform(jax.random.fold_in(own, axis_at), (blocks,), jnp.float32, low / len(cuts), high / len(cuts)))
        loudness = loudness * jnp.repeat(heights, dims[axis_at] // blocks).reshape([-1 if axis == axis_at else 1 for axis in range(len(dims))])
    return loudness


def noise(stream_key, extent, spread, most, split=(), dtype=jnp.bfloat16):
    result = jax.random.normal(stream_key, extent, jnp.float32) * spread
    if len(split) > 0:
        result = shard_levels(stream_key, extent, split, -0.22, 0.18) * result
    return jnp.clip(result, min=-most, max=most).astype(dtype)


def heavy_noise(stream_key, extent, spread, reach, pieces, heavy, kind=jnp.bfloat16):
    result = spread * jax.random.normal(stream_key, extent, jnp.float32)
    if pieces:
        result = result * shard_levels(stream_key, extent, pieces, -0.22, 0.18)
    return jnp.clip(spiked(result, jax.random.fold_in(stream_key, 3), *heavy), -reach, reach).astype(kind)


def setup_inputs(seed: int = 0) -> dict:
    splits = jax.random.split(jax.random.key(seed), 5)
    train_gate = heavy_noise(splits[0], (EXPERTS, D_MODEL, D_EXPERT), D_MODEL ** -0.5, 0.1875, ((0, 4), (1, 8)), (1, 2, 8, 2.0), jnp.float32)
    train_up = heavy_noise(splits[1], (EXPERTS, D_MODEL, D_EXPERT), D_MODEL ** -0.5, 0.1875, ((0, 4), (1, 8)), (1, 2, 8, 2.0), jnp.float32)
    router_weight = noise(splits[2], (D_MODEL, EXPERTS), D_MODEL ** -0.5, 0.125, ((0, 8), (1, 4)), jnp.float32)
    router_gain = jnp.clip(1.0 + 0.15 * jax.random.normal(splits[3], (D_MODEL,), jnp.float32), 0.25, 1.75)
    return dict(train_gate=train_gate, train_up=train_up, router_weight=router_weight, router_gain=router_gain)


def reference(train_gate, train_up, router_weight, router_gain):
    scale_gate = jnp.sqrt(lax.optimization_barrier(jnp.sum(train_gate * train_gate, axis=1)))
    ready_gate = (train_gate / jnp.expand_dims(scale_gate, 1)).astype(jnp.bfloat16)
    scale_up = jnp.sqrt(lax.optimization_barrier(jnp.sum(train_up * train_up, axis=1)))
    ready_up = (train_up / jnp.expand_dims(scale_up, 1)).astype(jnp.bfloat16)
    serve_router = (router_weight * router_gain[:, None]).astype(jnp.bfloat16)
    return (ready_gate, ready_up, scale_gate, scale_up, serve_router)
```

```python
import jax
import jax.numpy as jnp
from jax import lax
from jax.experimental import pallas as pl
from jax.experimental.pallas import tpu as pltpu
from jax.sharding import PartitionSpec as P


def tied(value, *others):
    return lax.optimization_barrier((value, *others))[0]


def shift(value, k):
    n = lax.axis_size("rows")
    return lax.ppermute(value, "rows", [(r, r ^ k) for r in range(n)])


def squares(x):
    return jnp.sum(x * x, axis=2)


def at(x, index):
    return lax.dynamic_index_in_dim(x, index, axis=0, keepdims=False)


def scaled(x, scale):
    return (x / scale[:, None, :]).astype(jnp.bfloat16)


def own_kernel(me_ref, x_ref, scale_ref, out_ref):
    del me_ref
    out_ref[...] = (x_ref[0] / scale_ref[...]).astype(jnp.bfloat16)


def own_piece(x, scale, me):
    n, per, rows, cols = x.shape
    return pl.pallas_call(
        own_kernel,
        grid_spec=pltpu.PrefetchScalarGridSpec(
            num_scalar_prefetch=1,
            grid=(per,),
            in_specs=[
                pl.BlockSpec((1, 1, rows, cols), lambda j, me: (me[0], j, 0, 0)),
                pl.BlockSpec((1, 1, cols), lambda j, me: (j, 0, 0)),
            ],
            out_specs=pl.BlockSpec((1, rows, cols), lambda j, me: (j, me[0], 0)),
        ),
        out_shape=jax.ShapeDtypeStruct((per, n * rows, cols), jnp.bfloat16),
        name="own",
    )(me[None], x, scale[:, None, :])


def place_kernel(source_ref, piece_ref, result_ref, out_ref):
    del source_ref, result_ref
    out_ref[...] = piece_ref[...]


def placed(result, piece, first, source):
    count, rows, cols = piece.shape
    return pl.pallas_call(
        place_kernel,
        grid_spec=pltpu.PrefetchScalarGridSpec(
            num_scalar_prefetch=1,
            grid=(count,),
            in_specs=[
                pl.BlockSpec((1, rows, cols), lambda j, s: (j, 0, 0)),
                pl.BlockSpec(memory_space=pl.ANY),
            ],
            out_specs=pl.BlockSpec(
                (1, rows, cols), lambda j, s: (first + j, s[0], 0)
            ),
        ),
        out_shape=jax.ShapeDtypeStruct(result.shape, result.dtype),
        input_output_aliases={2: 0},
        name="place",
    )(source[None], piece, result)


def gathered_router(weight, gain):
    n = lax.axis_size("rows")
    me = lax.axis_index("rows")
    held = (weight * gain[:, None]).astype(jnp.bfloat16)
    bit, depth = n // 2, 0
    while bit:
        other = shift(held, bit)
        low = (me & bit) == 0
        held = jnp.stack(
            [jnp.where(low, held, other), jnp.where(low, other, held)], axis=depth
        )
        bit, depth = bit // 2, depth + 1
    return held.reshape((-1, weight.shape[1]))


def groups(n):
    near = list(range(1, n // 2))
    far = list(range(n // 2, n))
    half, part = n // 4, n // 8
    return near, far, far[:half], far[half : half + part], far[half + part :]


def on_device(train_gate, train_up, router_weight, router_gain):
    n = lax.axis_size("rows")
    me = lax.axis_index("rows")
    experts, rows, cols = train_gate.shape
    per = experts // n
    gate = train_gate.reshape((n, per, rows, cols))
    up = train_up.reshape((n, per, rows, cols))
    near, far, far_a, far_b, far_c = groups(n)

    first = squares(gate[:, :1]).reshape((n, cols))
    parts = lax.all_to_all(
        jnp.broadcast_to(first[None], (n, n, cols)),
        "rows",
        split_axis=0,
        concat_axis=0,
        tiled=True,
    )
    first_scale = jnp.sqrt(jnp.sum(parts.reshape((n, n, cols)), axis=0))

    got_first = {}

    def send_first(ks, scales):
        last = None
        for k in ks:
            index = me ^ k if last is None else tied(me ^ k, last)
            last = scaled(at(gate, index)[:1], at(scales, index)[None])
            got_first[k] = shift(last, k)
        return last

    last = send_first(far_a, first_scale)
    last = send_first(near, tied(first_scale, last))

    gate_later, up_later, weight = tied((gate, up, router_weight), last)
    router = gathered_router(weight, router_gain)
    sums_gate = squares(gate_later[:, 1:])
    sums_up = squares(up_later)
    sums = jnp.concatenate([sums_gate, sums_up], axis=1)
    last = send_first(far_b + far_c, tied(first_scale, last))
    mine = [at(sums, me)] + [shift(at(sums, me ^ k), k) for k in far + near]
    scale = jnp.sqrt(sum(mine[1:], mine[0]))

    theirs = {k: shift(scale, k) for k in far + near}
    got_gate, got_up = {}, {}
    for k in far + near:
        if per > 1:
            last = scaled(at(gate, me ^ k)[1:], tied(theirs[k], last)[: per - 1])
            got_gate[k] = shift(last, k)
    for k in near + far:
        last = scaled(at(up, me ^ k), tied(theirs[k], last)[per - 1 :])
        got_up[k] = shift(last, k)

    scale, first_scale = tied((scale, first_scale), last)
    scale_gate = jnp.concatenate([at(first_scale, me)[None], scale[: per - 1]])
    scale_up = scale[per - 1 :]

    ready_gate = own_piece(gate, scale_gate, me)
    for k in far_a + near + far_b + far_c:
        ready_gate = placed(ready_gate, got_first[k], 0, me ^ k)
    ready_up = own_piece(up, scale_up, me)
    router = tied(router, ready_gate)
    serve_router = lax.all_gather(router, "owner", axis=1, tiled=True)
    if per > 1:
        for k in far + near:
            ready_gate = placed(ready_gate, got_gate[k], 1, me ^ k)
    for k in near + far:
        ready_up = placed(ready_up, got_up[k], 0, me ^ k)
    return (ready_gate, ready_up, scale_gate, scale_up, serve_router)


def solution(mesh):
    return jax.shard_map(
        on_device,
        mesh=mesh,
        in_specs=(
            P("owner", "rows", None),
            P("owner", "rows", None),
            P("rows", "owner"),
            P("rows"),
        ),
        out_specs=(
            P(("owner", "rows"), None, None),
            P(("owner", "rows"), None, None),
            P(("owner", "rows"), None),
            P(("owner", "rows"), None),
            P(),
        ),
        check_vma=False,
    )
```
